32 devices in a mesh: ka: 4 (over z), row: 8 (over y, x, core).
Axes of the slice: x: 2, y: 2, z: 4, core: 2. Of those that a mesh axis runs over, the one named last changes fastest.
Arguments:
- hamiltonian: float32 [16384, 4096], P(('ka', 'row')), parts along dimension 0, as said below
Outputs:
- sign_next: float32 [16384, 4096], P(('ka', 'row')), parts along dimension 0
- occupation: float32 [4], P('ka'), parts along dimension 0
There are 4 independent parts, one for each index of `ka`. The reference program is written for one: setup_inputs(seed, part) draws one part's arguments, and reference() takes and returns one part's arrays. A program takes and returns all parts, laid end to end along the dimension named above; each array names one. Nothing has to cross between parts.
Inputs may be any that keep to these rules, and one draw needn't show every extreme that they name: hamiltonian is symmetric up to float32 rounding.
All inputs are finite; a program needn't handle non-finite values.
Results may differ from the reference program's by a relative error of at most 0.0038.
Values may be sent and summed in bfloat16 or wider, within the bound.
A program may use at most 128 MiB of HBM per device.

```python
import math
import jax
import jax.numpy as jnp

N = 4096


def draw_hamiltonian(key, part):
    subkeys = jax.random.split(key, 4)
    channel_size = N // 2
    positions = jnp.arange(N, dtype=jnp.int32)
    ramped = positions.astype(jnp.float32) / N
    onsite = -0.3 + 1.2 * ramped + 0.15 * jax.random.normal(subkeys[0], (N,), jnp.float32)
    disorder = jax.random.normal(subkeys[1], (N, N), jnp.float32)
    hopping = 0.25 * (0.6 + 0.8 * jax.random.uniform(subkeys[2], (N - 1,), jnp.float32))
    inside = ((positions[:-1] + 1) % channel_size != 0).astype(jnp.float32)
    hopping = hopping * inside
    coupling = 0.25 * (0.6 + 0.8 * jax.random.uniform(subkeys[3], (channel_size,), jnp.float32))
    disorder = disorder * (0.3 / math.sqrt(2.0 * N))
    couplings = jnp.diag(hopping, 1) + jnp.diag(coupling, channel_size)
    return jnp.diag(onsite) + couplings + couplings.T + disorder + disorder.T


def setup_inputs(seed: int = 0, part: int = 0) -> dict:
    splits = jax.random.split(jax.random.key(seed), 2)
    part_splits = jax.random.split(jax.random.fold_in(splits[1], part), 2)
    hamiltonian = draw_hamiltonian(jax.random.fold_in(jax.random.fold_in(splits[1], part), 71), part)
    return dict(hamiltonian=hamiltonian)


def reference(hamiltonian):
    rounded = hamiltonian.astype(jnp.bfloat16)
    square = jnp.dot(rounded, rounded, preferred_element_type=jnp.float32).astype(jnp.bfloat16)
    cube = jnp.dot(square, rounded, preferred_element_type=jnp.float32)
    sign_next = 1.5 * hamiltonian - 0.5 * cube
    total = jnp.trace(sign_next)
    occupation = jnp.reshape(0.5 - total / (2.0 * N), (1,))
    return sign_next, occupation
```

```python
from functools import partial

import jax
import jax.numpy as jnp
from jax import lax
from jax.experimental import pallas as pl
from jax.experimental.pallas import tpu as pltpu
from jax.sharding import PartitionSpec as P

MESH = pl.DeviceIdType.MESH
PLANE = (2, 2, 2)
MESSAGES = 6


def multiply_rows(left, gathered):
    return jnp.dot(left, gathered, preferred_element_type=jnp.float32)


def own_diagonal(matrix, position, block_rows, cycle_size):
    shaped = matrix.reshape(block_rows, cycle_size, block_rows)
    square_block = lax.dynamic_slice_in_dim(shaped, position, 1, 1)[:, 0, :]
    return jnp.sum(jnp.diagonal(square_block))


def gathered_shards(hamiltonian):
    cycle_size = lax.axis_size("row")
    position = lax.axis_index("row")
    block_rows, order = hamiltonian.shape
    rounded = hamiltonian.astype(jnp.bfloat16)
    gathered = lax.all_gather(rounded, "row", axis=0, tiled=True)
    multiply = partial(multiply_rows, gathered=gathered)
    square_low = multiply(rounded).astype(jnp.bfloat16)
    cube = multiply(square_low)
    sign_next = 1.5 * hamiltonian - 0.5 * cube
    total = lax.psum(own_diagonal(sign_next, position, block_rows, cycle_size), "row")
    occupation = jnp.reshape(0.5 - total / (2.0 * order), (1,))
    return (sign_next, occupation)


def kernel(
    rounded_hbm, ham_hbm, out_hbm, occ_ref,
    g, s_low, s_acc, c_acc, tr,
    load_sem, out_sem, p_send, p_recv, x_send, x_recv, y_send, y_recv,
    f_send, f_recv, dx_send, dx_recv, dy_send, dy_recv, df_send, df_recv,
    t_send, t_recv,
):
    nb, order = rounded_hbm.shape
    half, wide, tile = nb // 2, 2 * nb, nb // 2
    pos = lax.axis_index("row")
    n_dev = lax.axis_size("row")
    chip, core = pos // 2, pos % 2
    y, x = chip // 2, chip % 2

    def chip_at(ry, rx, base=None):
        by, bx = (y, x) if base is None else base
        return (by + ry - 2 * by * ry, bx + rx - 2 * bx * rx)

    def index(at):
        return at[0] * 2 + at[1]

    here = (y, x)
    near_x, near_y, far = chip_at(0, 1), chip_at(1, 0), chip_at(1, 1)
    partner = pos + 1 - 2 * core

    def al(v, m=tile):
        return pl.multiple_of(v, m)

    def loc(axis, m, at, a):
        c = index(at)
        mine = (2 * c + a) * nb
        if m == 0:
            other = index(chip_at(1, 1, at))
            col = (2 * other + (a if axis == "x" else 1 - a)) * nb
            return pl.ds(al(mine), nb), pl.ds(al(col), nb)
        if m == 1:
            return pl.ds(al(mine), half), pl.ds(al(mine), nb)
        if m == 2:
            return pl.ds(al(mine + half), half), pl.ds(al(mine + half), half)
        if m == 3:
            return (
                pl.ds(al(2 * c * nb + a * half), half),
                pl.ds(al((2 * c + 1) * nb), nb),
            )
        other = index(chip_at(1, 0, at) if axis == "x" else chip_at(0, 1, at))
        return pl.ds(al(mine), nb), pl.ds(al((2 * other + m - 4) * nb), nb)

    def copy(where, target, send, recv):
        ref = g.at[where[0], where[1]]
        return pltpu.make_async_remote_copy(
            src_ref=ref, dst_ref=ref, send_sem=send, recv_sem=recv,
            device_id={"row": target}, device_id_type=MESH,
        )

    to_x = 2 * index(near_x) + core
    to_y = 2 * index(near_y) + core
    pass_from = (
        near_x[0] + core * (near_y[0] - near_x[0]),
        near_x[1] + core * (near_y[1] - near_x[1]),
    )
    to_pass = to_y + core * (to_x - to_y)

    def own(axis, m):
        sems = (x_send, x_recv) if axis == "x" else (y_send, y_recv)
        return copy(loc(axis, m, here, core), to_x if axis == "x" else to_y,
                    sems[0].at[m], sems[1].at[m])

    def arriving(axis, m):
        sems = (x_send, x_recv) if axis == "x" else (y_send, y_recv)
        return copy(loc(axis, m, near_x if axis == "x" else near_y, core),
                    to_x if axis == "x" else to_y, sems[0].at[m], sems[1].at[m])

    def shared(axis, m, a):
        sems = (dx_send, dx_recv) if axis == "x" else (dy_send, dy_recv)
        return copy(loc(axis, m, near_x if axis == "x" else near_y, a),
                    partner, sems[0].at[m], sems[1].at[m])

    def passed(m, at):
        return copy(loc("x", m, at, core), to_pass, f_send.at[m - 1], f_recv.at[m - 1])

    def passed_shared(m, a):
        return copy(loc("x", m, far, a), partner, df_send.at[m - 1], df_recv.at[m - 1])

    my_rows = pl.ds(al(pos * nb), nb)
    load = pltpu.make_async_copy(rounded_hbm, g.at[my_rows, :], load_sem.at[0])
    load.start()
    load_h = pltpu.make_async_copy(ham_hbm, c_acc, load_sem.at[1])
    load_h.start()
    barrier = pltpu.get_barrier_semaphore()
    for k in range(1, 8):
        pl.semaphore_signal(barrier, inc=1, device_id={"row": (pos + k) % n_dev},
                            device_id_type=MESH)
    pl.semaphore_wait(barrier, 7)
    load.wait()
    whole = copy((my_rows, slice(None)), partner, p_send, p_recv)
    for m in range(3):
        own("x", m).start()
        own("y", m).start()
    whole.start()

    f32 = jnp.float32

    def nn(left, right):
        return lax.dot_general(left, right, (((1,), (0,)), ((), ())),
                               preferred_element_type=f32)

    def nt(left, right):
        return lax.dot_general(left, right, (((1,), (1,)), ((), ())),
                               preferred_element_type=f32)

    left = g.at[my_rows, :]
    mine = pl.ds(al(pos * nb), nb)
    home = pl.ds(al(chip * wide), wide)
    load_h.wait()

    def eye():
        return (lax.broadcasted_iota(jnp.int32, (nb, nb), 0)
                == lax.broadcasted_iota(jnp.int32, (nb, nb), 1))

    tr_h = jnp.sum(jnp.where(eye(), c_acc[:, mine], 0.0), axis=0, keepdims=True)
    s_acc[0:1, mine] = tr_h

    whole_in = copy((pl.ds(al(partner * nb), nb), slice(None)), partner, p_send, p_recv)
    whole_in.wait_recv()
    for m in range(3, MESSAGES):
        own("x", m).start()
        own("y", m).start()
    tr[pos, 0:1, :] = s_acc[0:1, mine]

    @pl.loop(0, wide // tile)
    def _(t):
        at = al(chip * wide + t * tile)
        s_low[:, pl.ds(at, tile)] = nt(left[...], g[pl.ds(at, tile), :]).astype(jnp.bfloat16)

    def chip_rel(r):
        return chip_at(r // 2, r % 2)

    def forward_ready(axis, m):
        arriving(axis, m).wait_recv()
        shared(axis, m, core).start()

    per_chip = wide // tile

    @pl.loop(0, 3 * per_chip)
    def _(t):
        at = al(index(chip_rel(1 + t // per_chip)) * wide + (t % per_chip) * tile)
        s_acc[:, pl.ds(at, tile)] = nn(left[:, home], g[home, pl.ds(at, tile)])

    @pl.loop(0, order // tile)
    def _(t):
        cols = pl.ds(al(t * tile), tile)
        c_acc[:, cols] = -3.0 * c_acc[:, cols] + nn(s_low[:, home], g[home, cols])

    for m in range(3):
        forward_ready("x", m)
        forward_ready("y", m)
    for m in (1, 2):
        passed(m, pass_from).start()

    def add_pair(dst, lhs, i, j):
        rows, cols = pl.ds(al(i * nb), nb), pl.ds(al(j * nb), nb)
        dst[:, cols] += nn(lhs[:, rows], g[rows, cols])
        dst[:, rows] += nt(lhs[:, cols], g[rows, cols])

    nx, ny, nf = 2 * index(near_x), 2 * index(near_y), 2 * index(far)

    def add_cross(dst, lhs):
        @pl.loop(0, 4)
        def _(t):
            a, kind = t % 2, t // 2
            i = nx + a + kind * (ny - nx)
            j = ny + a + kind * (nx + 1 - a - ny - a)
            add_pair(dst, lhs, i, j)

    def add_diagonal(dst, lhs, base):
        rows = pl.ds(al(base * nb), wide)
        for t in range(per_chip):
            cols = pl.ds(al(base * nb + t * tile), tile)
            dst[:, cols] += nn(lhs[:, rows], g[rows, cols])

    def mirror_diagonal(base):
        low = al(base * nb)
        for b in range(2):
            at = low + b * nb
            g[pl.ds(al(at + half), half), pl.ds(al(at), half)] = (
                g[pl.ds(al(at), half), pl.ds(al(at + half), half)].T)
        for b in range(2):
            g[pl.ds(al(low + nb), nb), pl.ds(al(low + b * half), half)] = (
                g[pl.ds(al(low + b * half), half), pl.ds(al(low + nb), nb)].T)

    def wait_shared(m):
        shared("x", m, 1 - core).wait_recv()
        shared("y", m, 1 - core).wait_recv()

    wait_shared(0)
    add_cross(s_acc, left)
    forward_ready("x", 3)
    forward_ready("y", 3)
    passed(3, pass_from).start()
    for m in (1, 2, 3):
        wait_shared(m)

    @pl.loop(0, 2)
    def _(t):
        base = nx + t * (ny - nx)
        mirror_diagonal(base)
        add_diagonal(s_acc, left, base)

    for m in (4, 5):
        forward_ready("x", m)
        forward_ready("y", m)
        wait_shared(m)

        @pl.loop(0, 4)
        def _(t):
            i = nx + t % 2 + (t // 2) * (ny - nx)
            add_pair(s_acc, left, i, nf + m - 4)

    @pl.loop(0, 2)
    def _(t):
        base = nx + t * (ny - nx)
        part = pl.ds(al(base * nb), wide)
        s_low[:, part] = s_acc[:, part].astype(jnp.bfloat16)

    add_cross(c_acc, s_low)

    @pl.loop(0, 2)
    def _(t):
        base = nx + t * (ny - nx)
        part = pl.ds(al(base * nb), wide)
        add_diagonal(c_acc, s_low, base)
        for b in range(2):
            rows = pl.ds(al((2 * chip + b) * nb), nb)
            c_acc[:, rows] += nt(s_low[:, part], g[rows, part])
        for k in range(per_chip):
            cols = pl.ds(al(nf * nb + k * tile), tile)
            c_acc[:, cols] += nn(s_low[:, part], g[part, cols])

    for m in (1, 2, 3):
        passed(m, far).wait_recv()
        passed_shared(m, core).start()
    for m in (1, 2, 3):
        passed_shared(m, 1 - core).wait_recv()
    last = pl.ds(al(nf * nb), wide)
    mirror_diagonal(nf)
    add_diagonal(s_acc, left, nf)
    s_low[:, last] = s_acc[:, last].astype(jnp.bfloat16)

    def trace_step(t, carry):
        cols = pl.ds(al(t * nb), nb)
        product = s_low[:, cols].astype(f32) * left[:, cols].astype(f32)
        return carry + jnp.sum(product, axis=0, keepdims=True)

    tr_c = lax.fori_loop(0, order // nb, trace_step, jnp.zeros((1, nb), f32))
    tr[pos, 0:1, :] = 1.5 * tr[pos, 0:1, :] - 0.5 * tr_c

    def finish(i):
        cols = pl.ds(al(i * nb), nb)
        return pltpu.make_async_copy(c_acc.at[:, cols], out_hbm.at[:, cols], out_sem.at[i])

    for b in range(2):
        cols = pl.ds(al((nf + b) * nb), nb)
        c_acc[:, cols] = -0.5 * (c_acc[:, cols] + nn(s_low[:, last], g[last, cols]))
        finish(nf + b).start()

    def trace_copy(k, slot):
        return pltpu.make_async_remote_copy(
            src_ref=tr.at[slot], dst_ref=tr.at[slot],
            send_sem=t_send.at[k - 1], recv_sem=t_recv.at[k - 1],
            device_id={"row": (pos + k) % n_dev}, device_id_type=MESH,
        )

    for k in range(1, 8):
        trace_copy(k, pos).start()

    @pl.loop(0, 6)
    def _(t):
        i = 2 * index(chip_rel(t // 2)) + t % 2
        rows = pl.ds(al(i * nb), nb)
        c_acc[:, rows] = -0.5 * (c_acc[:, rows] + nt(s_low[:, last], g[rows, last]))
        finish(i).start()

    for k in range(1, 8):
        trace_copy(k, (pos + n_dev - k) % n_dev).wait_recv()
    total = jnp.sum(tr[:, 0:1, :])
    occ_ref[...] = jnp.full(occ_ref.shape, 0.5 - total / (2.0 * order), f32)

    for k in range(1, 8):
        trace_copy(k, pos).wait_send()
    whole.wait_send()
    for m in range(MESSAGES):
        for axis in ("x", "y"):
            own(axis, m).wait_send()
            shared(axis, m, core).wait_send()
    for m in (1, 2, 3):
        passed(m, pass_from).wait_send()
        passed_shared(m, core).wait_send()

    @pl.loop(0, order // nb)
    def _(i):
        finish(i).wait()


def symmetric_shards(hamiltonian):
    nb, order = hamiltonian.shape
    cycle_size = lax.axis_size("row")
    dma = pltpu.SemaphoreType.DMA
    six, three, seven = dma((MESSAGES,)), dma((3,)), dma((cycle_size - 1,))
    hbm = pl.BlockSpec(memory_space=pl.ANY)
    sign_next, occupation = pl.pallas_call(
        kernel,
        out_shape=(
            jax.ShapeDtypeStruct((nb, order), jnp.float32),
            jax.ShapeDtypeStruct((8, 128), jnp.float32),
        ),
        in_specs=[hbm, hbm],
        out_specs=(hbm, pl.BlockSpec(memory_space=pltpu.VMEM)),
        scratch_shapes=[
            pltpu.VMEM((order, order), jnp.bfloat16),
            pltpu.VMEM((nb, order), jnp.bfloat16),
            pltpu.VMEM((nb, order), jnp.float32),
            pltpu.VMEM((nb, order), jnp.float32),
            pltpu.VMEM((cycle_size, 8, nb), jnp.float32),
            dma((2,)), dma((cycle_size,)), dma, dma,
            six, six, six, six, three, three,
            six, six, six, six, three, three,
            seven, seven,
        ],
        compiler_params=pltpu.CompilerParams(
            collective_id=0, has_side_effects=True, vmem_limit_bytes=67043328,
        ),
    )(hamiltonian.astype(jnp.bfloat16), hamiltonian)
    return (sign_next, occupation[0, :1])


def solution(mesh):
    plane = PLANE[0] * PLANE[1] * PLANE[2]
    shards = symmetric_shards if mesh.shape["row"] == plane else gathered_shards
    placed = (P(("ka", "row"), None),)
    return jax.shard_map(
        shards,
        mesh=mesh,
        in_specs=placed,
        out_specs=(P(("ka", "row"), None), P("ka")),
        check_vma=False,
    )
```

```python
from functools import partial

import jax
import jax.numpy as jnp
from jax import lax
from jax.experimental import pallas as pl
from jax.experimental.pallas import tpu as pltpu
from jax.sharding import PartitionSpec as P

MESH = pl.DeviceIdType.MESH
PLANE = (2, 2, 2)
MESSAGES = 6


def multiply_rows(left, gathered):
    return jnp.dot(left, gathered, preferred_element_type=jnp.float32)


def own_diagonal(matrix, position, block_rows, cycle_size):
    shaped = matrix.reshape(block_rows, cycle_size, block_rows)
    square_block = lax.dynamic_slice_in_dim(shaped, position, 1, 1)[:, 0, :]
    return jnp.sum(jnp.diagonal(square_block))


def gathered_shards(hamiltonian):
    cycle_size = lax.axis_size("row")
    position = lax.axis_index("row")
    block_rows, order = hamiltonian.shape
    rounded = hamiltonian.astype(jnp.bfloat16)
    gathered = lax.all_gather(rounded, "row", axis=0, tiled=True)
    multiply = partial(multiply_rows, gathered=gathered)
    square_low = multiply(rounded).astype(jnp.bfloat16)
    cube = multiply(square_low)
    sign_next = 1.5 * hamiltonian - 0.5 * cube
    total = lax.psum(own_diagonal(sign_next, position, block_rows, cycle_size), "row")
    occupation = jnp.reshape(0.5 - total / (2.0 * order), (1,))
    return (sign_next, occupation)


def kernel(
    ham_hbm, c_acc, occ_ref,
    g, s_low, s_acc, tr,
    load_sem, p_send, p_recv, x_send, x_recv, y_send, y_recv,
    f_send, f_recv, dx_send, dx_recv, dy_send, dy_recv, df_send, df_recv,
    t_send, t_recv,
):
    nb, order = ham_hbm.shape
    half, wide, tile = nb // 2, 2 * nb, nb // 2
    pos = lax.axis_index("row")
    n_dev = lax.axis_size("row")
    chip, core = pos // 2, pos % 2
    y, x = chip // 2, chip % 2

    def chip_at(ry, rx, base=None):
        by, bx = (y, x) if base is None else base
        return (by + ry - 2 * by * ry, bx + rx - 2 * bx * rx)

    def index(at):
        return at[0] * 2 + at[1]

    here = (y, x)
    near_x, near_y, far = chip_at(0, 1), chip_at(1, 0), chip_at(1, 1)
    partner = pos + 1 - 2 * core

    def al(v, m=tile):
        return pl.multiple_of(v, m)

    def loc(axis, m, at, a):
        c = index(at)
        mine = (2 * c + a) * nb
        if m == 0:
            other = index(chip_at(1, 1, at))
            col = (2 * other + (a if axis == "x" else 1 - a)) * nb
            return pl.ds(al(mine), nb), pl.ds(al(col), nb)
        if m == 1:
            return pl.ds(al(mine), half), pl.ds(al(mine), nb)
        if m == 2:
            return pl.ds(al(mine + half), half), pl.ds(al(mine + half), half)
        if m == 3:
            return (
                pl.ds(al(2 * c * nb + a * half), half),
                pl.ds(al((2 * c + 1) * nb), nb),
            )
        other = index(chip_at(1, 0, at) if axis == "x" else chip_at(0, 1, at))
        row = (2 * c + m - 4) * nb + a * half
        return pl.ds(al(row), half), pl.ds(al(other * wide), wide)

    def copy(where, target, send, recv):
        ref = g.at[where[0], where[1]]
        return pltpu.make_async_remote_copy(
            src_ref=ref, dst_ref=ref, send_sem=send, recv_sem=recv,
            device_id={"row": target}, device_id_type=MESH,
        )

    to_x = 2 * index(near_x) + core
    to_y = 2 * index(near_y) + core
    pass_from = (
        near_x[0] + core * (near_y[0] - near_x[0]),
        near_x[1] + core * (near_y[1] - near_x[1]),
    )
    to_pass = to_y + core * (to_x - to_y)

    def own(axis, m):
        sems = (x_send, x_recv) if axis == "x" else (y_send, y_recv)
        return copy(loc(axis, m, here, core), to_x if axis == "x" else to_y,
                    sems[0].at[m], sems[1].at[m])

    def arriving(axis, m):
        sems = (x_send, x_recv) if axis == "x" else (y_send, y_recv)
        return copy(loc(axis, m, near_x if axis == "x" else near_y, core),
                    to_x if axis == "x" else to_y, sems[0].at[m], sems[1].at[m])

    def shared(axis, m, a):
        sems = (dx_send, dx_recv) if axis == "x" else (dy_send, dy_recv)
        return copy(loc(axis, m, near_x if axis == "x" else near_y, a),
                    partner, sems[0].at[m], sems[1].at[m])

    def passed(m, at):
        return copy(loc("x", m, at, core), to_pass, f_send.at[m - 1], f_recv.at[m - 1])

    def passed_shared(m, a):
        return copy(loc("x", m, far, a), partner, df_send.at[m - 1], df_recv.at[m - 1])

    my_rows = pl.ds(al(pos * nb), nb)
    pieces = []
    for k, at in enumerate((far, here, near_x, near_y)):
        cols = pl.ds(al(index(at) * wide), wide)
        load = pltpu.make_async_copy(ham_hbm.at[:, cols], c_acc.at[:, cols], load_sem.at[k])
        load.start()
        pieces.append((cols, load))

    def round_piece(k):
        cols, load = pieces[k]
        load.wait()

        @pl.loop(0, nb // 32)
        def _(t):
            rows = pl.ds(pl.multiple_of(t * 32, 32), 32)
            to = pl.ds(pl.multiple_of(pos * nb + t * 32, 32), 32)
            g[to, cols] = c_acc[rows, cols].astype(jnp.bfloat16)

    barrier = pltpu.get_barrier_semaphore()
    for k in range(1, 8):
        pl.semaphore_signal(barrier, inc=1, device_id={"row": (pos + k) % n_dev},
                            device_id_type=MESH)
    round_piece(0)
    round_piece(1)
    pl.semaphore_wait(barrier, 7)
    own("x", 0).start()
    own("y", 0).start()
    round_piece(2)
    round_piece(3)
    for m in (1, 2):
        own("x", m).start()
        own("y", m).start()
    whole = copy((my_rows, slice(None)), partner, p_send, p_recv)
    whole.start()

    f32 = jnp.float32

    def nn(left, right):
        return lax.dot_general(left, right, (((1,), (0,)), ((), ())),
                               preferred_element_type=f32)

    def nt(left, right):
        return lax.dot_general(left, right, (((1,), (1,)), ((), ())),
                               preferred_element_type=f32)

    left = g.at[my_rows, :]
    mine = pl.ds(al(pos * nb), nb)
    home = pl.ds(al(chip * wide), wide)

    def eye():
        return (lax.broadcasted_iota(jnp.int32, (nb, nb), 0)
                == lax.broadcasted_iota(jnp.int32, (nb, nb), 1))

    tr_h = jnp.sum(jnp.where(eye(), c_acc[:, mine], 0.0), axis=0, keepdims=True)
    s_acc[0:1, mine] = tr_h

    whole_in = copy((pl.ds(al(partner * nb), nb), slice(None)), partner, p_send, p_recv)
    whole_in.wait_recv()
    for m in range(3, MESSAGES):
        own("x", m).start()
        own("y", m).start()
    tr[pos, 0:1, :] = s_acc[0:1, mine]

    @pl.loop(0, wide // tile)
    def _(t):
        at = al(chip * wide + t * tile)
        s_low[:, pl.ds(at, tile)] = nt(left[...], g[pl.ds(at, tile), :]).astype(jnp.bfloat16)

    def chip_rel(r):
        return chip_at(r // 2, r % 2)

    def forward_ready(axis, m):
        arriving(axis, m).wait_recv()
        shared(axis, m, core).start()

    per_chip = wide // tile

    @pl.loop(0, 3 * per_chip)
    def _(t):
        at = al(index(chip_rel(1 + t // per_chip)) * wide + (t % per_chip) * tile)
        s_acc[:, pl.ds(at, tile)] = nn(left[:, home], g[home, pl.ds(at, tile)])

    @pl.loop(0, order // tile)
    def _(t):
        cols = pl.ds(al(t * tile), tile)
        c_acc[:, cols] = -3.0 * c_acc[:, cols] + nn(s_low[:, home], g[home, cols])

    for m in range(3):
        forward_ready("x", m)
        forward_ready("y", m)
    for m in (1, 2):
        passed(m, pass_from).start()

    def add_pair(dst, lhs, i, j):
        rows, cols = pl.ds(al(i * nb), nb), pl.ds(al(j * nb), nb)
        dst[:, cols] += nn(lhs[:, rows], g[rows, cols])
        dst[:, rows] += nt(lhs[:, cols], g[rows, cols])

    nx, ny, nf = 2 * index(near_x), 2 * index(near_y), 2 * index(far)

    def add_cross(dst, lhs):
        @pl.loop(0, 4)
        def _(t):
            a, kind = t % 2, t // 2
            i = nx + a + kind * (ny - nx)
            j = ny + a + kind * (nx + 1 - a - ny - a)
            add_pair(dst, lhs, i, j)

    def add_diagonal(dst, lhs, base):
        rows = pl.ds(al(base * nb), wide)
        for t in range(per_chip):
            cols = pl.ds(al(base * nb + t * tile), tile)
            dst[:, cols] += nn(lhs[:, rows], g[rows, cols])

    def mirror_diagonal(base):
        low = al(base * nb)
        for b in range(2):
            at = low + b * nb
            g[pl.ds(al(at + half), half), pl.ds(al(at), half)] = (
                g[pl.ds(al(at), half), pl.ds(al(at + half), half)].T)
        for b in range(2):
            g[pl.ds(al(low + nb), nb), pl.ds(al(low + b * half), half)] = (
                g[pl.ds(al(low + b * half), half), pl.ds(al(low + nb), nb)].T)

    def wait_shared(m):
        shared("x", m, 1 - core).wait_recv()
        shared("y", m, 1 - core).wait_recv()

    wait_shared(0)
    add_cross(s_acc, left)
    forward_ready("x", 3)
    forward_ready("y", 3)
    passed(3, pass_from).start()
    for m in (1, 2, 3):
        wait_shared(m)

    @pl.loop(0, 2)
    def _(t):
        base = nx + t * (ny - nx)
        mirror_diagonal(base)
        add_diagonal(s_acc, left, base)

    def block(k):
        return pl.ds(al(k * nb), nb)

    def add_column(q, base):
        for k in range(2):
            to = block(2 * chip + k)
            c_acc[:, to] += nt(s_low[:, block(q)], g[to, block(q)])
        for start in (nf, base):
            for k in range(2):
                to = block(start + k)
                c_acc[:, to] += nn(s_low[:, block(q)], g[block(q), to])

    for b in range(2):
        forward_ready("x", 4 + b)
        forward_ready("y", 4 + b)
        wait_shared(4 + b)

        @pl.loop(0, 4)
        def _(t):
            add_pair(s_acc, left, nx + b + (t // 2) * (ny - nx), nf + t % 2)

        qx, qy = nx + b, ny + b
        for q in (qx, qy):
            s_low[:, block(q)] = s_acc[:, block(q)].astype(jnp.bfloat16)
        c_acc[:, block(qy)] += nn(s_low[:, block(qx)], g[block(qx), block(qy)])
        c_acc[:, block(qx)] += nt(s_low[:, block(qy)], g[block(qx), block(qy)])
        c_acc[:, block(ny + 1 - b)] += nt(
            s_low[:, block(qx)], g[block(ny + 1 - b), block(qx)])
        c_acc[:, block(nx + 1 - b)] += nn(
            s_low[:, block(qy)], g[block(qy), block(nx + 1 - b)])
        if b == 0:
            @pl.loop(0, 2)
            def _(t):
                base = nx + t * (ny - nx)
                add_column(base + b, base)
        else:
            add_column(nx + b, nx)
            for m in (1, 2, 3):
                passed(m, far).wait_recv()
                passed_shared(m, core).start()
            add_column(ny + b, ny)

    for m in (1, 2, 3):
        passed_shared(m, 1 - core).wait_recv()
    last = pl.ds(al(nf * nb), wide)
    mirror_diagonal(nf)
    add_diagonal(s_acc, left, nf)
    s_low[:, last] = s_acc[:, last].astype(jnp.bfloat16)

    def trace_step(t, carry):
        cols = pl.ds(al(t * nb), nb)
        product = s_low[:, cols].astype(f32) * left[:, cols].astype(f32)
        return carry + jnp.sum(product, axis=0, keepdims=True)

    tr_c = lax.fori_loop(0, order // nb, trace_step, jnp.zeros((1, nb), f32))
    tr[pos, 0:1, :] = 1.5 * tr[pos, 0:1, :] - 0.5 * tr_c

    for b in range(2):
        cols = pl.ds(al((nf + b) * nb), nb)
        c_acc[:, cols] = -0.5 * (c_acc[:, cols] + nn(s_low[:, last], g[last, cols]))

    def trace_copy(k, slot):
        return pltpu.make_async_remote_copy(
            src_ref=tr.at[slot], dst_ref=tr.at[slot],
            send_sem=t_send.at[k - 1], recv_sem=t_recv.at[k - 1],
            device_id={"row": (pos + k) % n_dev}, device_id_type=MESH,
        )

    for k in range(1, 8):
        trace_copy(k, pos).start()

    @pl.loop(0, 6)
    def _(t):
        i = 2 * index(chip_rel(t // 2)) + t % 2
        rows = pl.ds(al(i * nb), nb)
        c_acc[:, rows] = -0.5 * (c_acc[:, rows] + nt(s_low[:, last], g[rows, last]))

    for k in range(1, 8):
        trace_copy(k, (pos + n_dev - k) % n_dev).wait_recv()
    total = jnp.sum(tr[:, 0:1, :])
    occ_ref[...] = jnp.full(occ_ref.shape, 0.5 - total / (2.0 * order), f32)

    for k in range(1, 8):
        trace_copy(k, pos).wait_send()
    whole.wait_send()
    for m in range(MESSAGES):
        for axis in ("x", "y"):
            own(axis, m).wait_send()
            shared(axis, m, core).wait_send()
    for m in (1, 2, 3):
        passed(m, pass_from).wait_send()
        passed_shared(m, core).wait_send()


def symmetric_shards(hamiltonian):
    nb, order = hamiltonian.shape
    cycle_size = lax.axis_size("row")
    dma = pltpu.SemaphoreType.DMA
    six, three, seven = dma((MESSAGES,)), dma((3,)), dma((cycle_size - 1,))
    hbm = pl.BlockSpec(memory_space=pl.ANY)
    sign_next, occupation = pl.pallas_call(
        kernel,
        out_shape=(
            pltpu.VMEM((nb, order), jnp.float32),
            jax.ShapeDtypeStruct((8, 128), jnp.float32),
        ),
        in_specs=[hbm],
        out_specs=(pl.BlockSpec(memory_space=pltpu.VMEM), pl.BlockSpec(memory_space=pltpu.VMEM)),
        scratch_shapes=[
            pltpu.VMEM((order, order), jnp.bfloat16),
            pltpu.VMEM((nb, order), jnp.bfloat16),
            pltpu.VMEM((nb, order), jnp.float32),
            pltpu.VMEM((cycle_size, 8, nb), jnp.float32),
            dma((4,)), dma, dma,
            six, six, six, six, three, three,
            six, six, six, six, three, three,
            seven, seven,
        ],
        compiler_params=pltpu.CompilerParams(
            collective_id=0, has_side_effects=True, vmem_limit_bytes=50 * 2**20,
        ),
    )(hamiltonian)
    return (sign_next, occupation[0, :1])


def solution(mesh):
    plane = PLANE[0] * PLANE[1] * PLANE[2]
    shards = symmetric_shards if mesh.shape["row"] == plane else gathered_shards
    placed = (P(("ka", "row"), None),)
    return jax.shard_map(
        shards,
        mesh=mesh,
        in_specs=placed,
        out_specs=(P(("ka", "row"), None), P("ka")),
        check_vma=False,
    )
```

```python
from functools import partial

import jax
import jax.numpy as jnp
from jax import lax
from jax.experimental import pallas as pl
from jax.experimental.pallas import tpu as pltpu
from jax.sharding import PartitionSpec as P

MESH = pl.DeviceIdType.MESH
PLANE = (2, 2, 2)
MESSAGES = 6


def multiply_rows(left, gathered):
    return jnp.dot(left, gathered, preferred_element_type=jnp.float32)


def own_diagonal(matrix, position, block_rows, cycle_size):
    shaped = matrix.reshape(block_rows, cycle_size, block_rows)
    square_block = lax.dynamic_slice_in_dim(shaped, position, 1, 1)[:, 0, :]
    return jnp.sum(jnp.diagonal(square_block))


def gathered_shards(hamiltonian):
    cycle_size = lax.axis_size("row")
    position = lax.axis_index("row")
    block_rows, order = hamiltonian.shape
    rounded = hamiltonian.astype(jnp.bfloat16)
    gathered = lax.all_gather(rounded, "row", axis=0, tiled=True)
    multiply = partial(multiply_rows, gathered=gathered)
    square_low = multiply(rounded).astype(jnp.bfloat16)
    cube = multiply(square_low)
    sign_next = 1.5 * hamiltonian - 0.5 * cube
    total = lax.psum(own_diagonal(sign_next, position, block_rows, cycle_size), "row")
    occupation = jnp.reshape(0.5 - total / (2.0 * order), (1,))
    return (sign_next, occupation)


def kernel(
    ham_hbm, c_acc, occ_ref,
    g, s_low, s_acc, tr,
    load_sem, p_send, p_recv, x_send, x_recv, y_send, y_recv,
    f_send, f_recv, dx_send, dx_recv, dy_send, dy_recv, df_send, df_recv,
    t_send, t_recv,
):
    nb, order = ham_hbm.shape
    half, wide, tile = nb // 2, 2 * nb, nb // 2
    pos = lax.axis_index("row")
    n_dev = lax.axis_size("row")
    chip, core = pos // 2, pos % 2
    y, x = chip // 2, chip % 2

    def chip_at(ry, rx, base=None):
        by, bx = (y, x) if base is None else base
        return (by + ry - 2 * by * ry, bx + rx - 2 * bx * rx)

    def index(at):
        return at[0] * 2 + at[1]

    here = (y, x)
    near_x, near_y, far = chip_at(0, 1), chip_at(1, 0), chip_at(1, 1)
    partner = pos + 1 - 2 * core

    def al(v, m=tile):
        return pl.multiple_of(v, m)

    def loc(axis, m, at, a):
        c = index(at)
        mine = (2 * c + a) * nb
        if m == 0:
            other = index(chip_at(1, 1, at))
            col = (2 * other + (a if axis == "x" else 1 - a)) * nb
            return pl.ds(al(mine), nb), pl.ds(al(col), nb)
        if m == 1:
            return pl.ds(al(mine), half), pl.ds(al(mine), nb)
        if m == 2:
            return pl.ds(al(mine + half), half), pl.ds(al(mine + half), half)
        if m == 3:
            return (
                pl.ds(al(2 * c * nb + a * half), half),
                pl.ds(al((2 * c + 1) * nb), nb),
            )
        other = index(chip_at(1, 0, at) if axis == "x" else chip_at(0, 1, at))
        row = (2 * c + m - 4) * nb + a * half
        return pl.ds(al(row), half), pl.ds(al(other * wide), wide)

    def copy(where, target, send, recv):
        ref = g.at[where[0], where[1]]
        return pltpu.make_async_remote_copy(
            src_ref=ref, dst_ref=ref, send_sem=send, recv_sem=recv,
            device_id={"row": target}, device_id_type=MESH,
        )

    to_x = 2 * index(near_x) + core
    to_y = 2 * index(near_y) + core
    pass_from = (
        near_x[0] + core * (near_y[0] - near_x[0]),
        near_x[1] + core * (near_y[1] - near_x[1]),
    )
    to_pass = to_y + core * (to_x - to_y)

    def own(axis, m):
        sems = (x_send, x_recv) if axis == "x" else (y_send, y_recv)
        return copy(loc(axis, m, here, core), to_x if axis == "x" else to_y,
                    sems[0].at[m], sems[1].at[m])

    def arriving(axis, m):
        sems = (x_send, x_recv) if axis == "x" else (y_send, y_recv)
        return copy(loc(axis, m, near_x if axis == "x" else near_y, core),
                    to_x if axis == "x" else to_y, sems[0].at[m], sems[1].at[m])

    def shared(axis, m, a):
        sems = (dx_send, dx_recv) if axis == "x" else (dy_send, dy_recv)
        return copy(loc(axis, m, near_x if axis == "x" else near_y, a),
                    partner, sems[0].at[m], sems[1].at[m])

    def passed(m, at):
        return copy(loc("x", m, at, core), to_pass, f_send.at[m - 1], f_recv.at[m - 1])

    def passed_shared(m, a):
        return copy(loc("x", m, far, a), partner, df_send.at[m - 1], df_recv.at[m - 1])

    my_rows = pl.ds(al(pos * nb), nb)
    pieces = []
    for k, at in enumerate((far, here, near_x, near_y)):
        cols = pl.ds(al(index(at) * wide), wide)
        load = pltpu.make_async_copy(ham_hbm.at[:, cols], c_acc.at[:, cols], load_sem.at[k])
        load.start()
        pieces.append((cols, load))

    def round_piece(k):
        cols, load = pieces[k]
        load.wait()

        @pl.loop(0, nb // 32)
        def _(t):
            rows = pl.ds(pl.multiple_of(t * 32, 32), 32)
            to = pl.ds(pl.multiple_of(pos * nb + t * 32, 32), 32)
            g[to, cols] = c_acc[rows, cols].astype(jnp.bfloat16)

    barrier = pltpu.get_barrier_semaphore()
    for k in range(1, 8):
        pl.semaphore_signal(barrier, inc=1, device_id={"row": (pos + k) % n_dev},
                            device_id_type=MESH)
    round_piece(0)
    round_piece(1)
    pl.semaphore_wait(barrier, 7)
    own("x", 0).start()
    own("y", 0).start()
    round_piece(2)
    round_piece(3)
    for m in (1, 2):
        own("x", m).start()
        own("y", m).start()
    whole = copy((my_rows, slice(None)), partner, p_send, p_recv)
    whole.start()

    f32 = jnp.float32

    def nn(left, right):
        return lax.dot_general(left, right, (((1,), (0,)), ((), ())),
                               preferred_element_type=f32)

    def nt(left, right):
        return lax.dot_general(left, right, (((1,), (1,)), ((), ())),
                               preferred_element_type=f32)

    left = g.at[my_rows, :]
    mine = pl.ds(al(pos * nb), nb)
    home = pl.ds(al(chip * wide), wide)

    def eye():
        return (lax.broadcasted_iota(jnp.int32, (nb, nb), 0)
                == lax.broadcasted_iota(jnp.int32, (nb, nb), 1))

    tr_h = jnp.sum(jnp.where(eye(), c_acc[:, mine], 0.0), axis=0, keepdims=True)
    s_acc[0:1, mine] = tr_h

    whole_in = copy((pl.ds(al(partner * nb), nb), slice(None)), partner, p_send, p_recv)
    whole_in.wait_recv()
    for m in range(3, MESSAGES):
        own("x", m).start()
        own("y", m).start()
    tr[pos, 0:1, :] = s_acc[0:1, mine]

    @pl.loop(0, wide // tile)
    def _(t):
        at = al(chip * wide + t * tile)
        s_low[:, pl.ds(at, tile)] = nt(left[...], g[pl.ds(at, tile), :]).astype(jnp.bfloat16)

    def chip_rel(r):
        return chip_at(r // 2, r % 2)

    def forward_ready(axis, m):
        arriving(axis, m).wait_recv()
        shared(axis, m, core).start()

    per_chip = wide // tile

    @pl.loop(0, 3 * per_chip)
    def _(t):
        at = al(index(chip_rel(1 + t // per_chip)) * wide + (t % per_chip) * tile)
        s_acc[:, pl.ds(at, tile)] = nn(left[:, home], g[home, pl.ds(at, tile)])

    @pl.loop(0, order // tile)
    def _(t):
        cols = pl.ds(al(t * tile), tile)
        c_acc[:, cols] = -3.0 * c_acc[:, cols] + nn(s_low[:, home], g[home, cols])

    for m in range(3):
        forward_ready("x", m)
        forward_ready("y", m)
    for m in (1, 2):
        passed(m, pass_from).start()

    def add_pair(dst, lhs, i, j):
        rows, cols = pl.ds(al(i * nb), nb), pl.ds(al(j * nb), nb)
        dst[:, cols] += nn(lhs[:, rows], g[rows, cols])
        dst[:, rows] += nt(lhs[:, cols], g[rows, cols])

    nx, ny, nf = 2 * index(near_x), 2 * index(near_y), 2 * index(far)

    def add_cross(dst, lhs):
        @pl.loop(0, 4)
        def _(t):
            a, kind = t % 2, t // 2
            i = nx + a + kind * (ny - nx)
            j = ny + a + kind * (nx + 1 - a - ny - a)
            add_pair(dst, lhs, i, j)

    def add_diagonal(dst, lhs, base):
        rows = pl.ds(al(base * nb), wide)
        for t in range(per_chip):
            cols = pl.ds(al(base * nb + t * tile), tile)
            dst[:, cols] += nn(lhs[:, rows], g[rows, cols])

    def mirror_diagonal(base):
        low = al(base * nb)
        for b in range(2):
            at = low + b * nb
            g[pl.ds(al(at + half), half), pl.ds(al(at), half)] = (
                g[pl.ds(al(at), half), pl.ds(al(at + half), half)].T)
        for b in range(2):
            g[pl.ds(al(low + nb), nb), pl.ds(al(low + b * half), half)] = (
                g[pl.ds(al(low + b * half), half), pl.ds(al(low + nb), nb)].T)

    def wait_shared(m):
        shared("x", m, 1 - core).wait_recv()
        shared("y", m, 1 - core).wait_recv()

    wait_shared(0)
    add_cross(s_acc, left)
    forward_ready("x", 3)
    forward_ready("y", 3)
    passed(3, pass_from).start()
    for m in (1, 2, 3):
        wait_shared(m)

    @pl.loop(0, 2)
    def _(t):
        base = nx + t * (ny - nx)
        mirror_diagonal(base)
        add_diagonal(s_acc, left, base)

    def block(k):
        return pl.ds(al(k * nb), nb)

    def add_column(q, base):
        for k in range(2):
            to = block(2 * chip + k)
            c_acc[:, to] += nt(s_low[:, block(q)], g[to, block(q)])
        for start in (nf, base):
            for k in range(2):
                to = block(start + k)
                c_acc[:, to] += nn(s_low[:, block(q)], g[block(q), to])

    def trace_step(t, carry):
        cols = block(2 * index(chip_rel(t // 2)) + t % 2)
        product = s_low[:, cols].astype(f32) * left[:, cols].astype(f32)
        return carry + jnp.sum(product, axis=0, keepdims=True)

    for b in range(2):
        forward_ready("x", 4 + b)
        forward_ready("y", 4 + b)
        wait_shared(4 + b)

        @pl.loop(0, 4)
        def _(t):
            add_pair(s_acc, left, nx + b + (t // 2) * (ny - nx), nf + t % 2)

        qx, qy = nx + b, ny + b
        for q in (qx, qy):
            s_low[:, block(q)] = s_acc[:, block(q)].astype(jnp.bfloat16)
        c_acc[:, block(qy)] += nn(s_low[:, block(qx)], g[block(qx), block(qy)])
        c_acc[:, block(qx)] += nt(s_low[:, block(qy)], g[block(qx), block(qy)])
        c_acc[:, block(ny + 1 - b)] += nt(
            s_low[:, block(qx)], g[block(ny + 1 - b), block(qx)])
        c_acc[:, block(nx + 1 - b)] += nn(
            s_low[:, block(qy)], g[block(qy), block(nx + 1 - b)])
        if b == 0:
            @pl.loop(0, 2)
            def _(t):
                base = nx + t * (ny - nx)
                add_column(base + b, base)
        else:
            add_column(nx + b, nx)
            tr_c = lax.fori_loop(0, 6, trace_step, jnp.zeros((1, nb), f32))
            for m in (1, 2, 3):
                passed(m, far).wait_recv()
                passed_shared(m, core).start()
            add_column(ny + b, ny)

    for m in (1, 2, 3):
        passed_shared(m, 1 - core).wait_recv()
    last = pl.ds(al(nf * nb), wide)
    mirror_diagonal(nf)
    add_diagonal(s_acc, left, nf)
    s_low[:, last] = s_acc[:, last].astype(jnp.bfloat16)

    tr_c = lax.fori_loop(6, 8, trace_step, tr_c)
    tr[pos, 0:1, :] = 1.5 * tr[pos, 0:1, :] - 0.5 * tr_c

    for b in range(2):
        cols = pl.ds(al((nf + b) * nb), nb)
        c_acc[:, cols] = -0.5 * (c_acc[:, cols] + nn(s_low[:, last], g[last, cols]))

    def trace_copy(k, slot):
        return pltpu.make_async_remote_copy(
            src_ref=tr.at[slot], dst_ref=tr.at[slot],
            send_sem=t_send.at[k - 1], recv_sem=t_recv.at[k - 1],
            device_id={"row": (pos + k) % n_dev}, device_id_type=MESH,
        )

    for k in range(1, 8):
        trace_copy(k, pos).start()

    @pl.loop(0, 6)
    def _(t):
        i = 2 * index(chip_rel(t // 2)) + t % 2
        rows = pl.ds(al(i * nb), nb)
        c_acc[:, rows] = -0.5 * (c_acc[:, rows] + nt(s_low[:, last], g[rows, last]))

    for k in range(1, 8):
        trace_copy(k, (pos + n_dev - k) % n_dev).wait_recv()
    total = jnp.sum(tr[:, 0:1, :])
    occ_ref[...] = jnp.full(occ_ref.shape, 0.5 - total / (2.0 * order), f32)

    for k in range(1, 8):
        trace_copy(k, pos).wait_send()
    whole.wait_send()
    for m in range(MESSAGES):
        for axis in ("x", "y"):
            own(axis, m).wait_send()
            shared(axis, m, core).wait_send()
    for m in (1, 2, 3):
        passed(m, pass_from).wait_send()
        passed_shared(m, core).wait_send()


def symmetric_shards(hamiltonian):
    nb, order = hamiltonian.shape
    cycle_size = lax.axis_size("row")
    dma = pltpu.SemaphoreType.DMA
    six, three, seven = dma((MESSAGES,)), dma((3,)), dma((cycle_size - 1,))
    hbm = pl.BlockSpec(memory_space=pl.ANY)
    sign_next, occupation = pl.pallas_call(
        kernel,
        out_shape=(
            pltpu.VMEM((nb, order), jnp.float32),
            jax.ShapeDtypeStruct((8, 128), jnp.float32),
        ),
        in_specs=[hbm],
        out_specs=(pl.BlockSpec(memory_space=pltpu.VMEM), pl.BlockSpec(memory_space=pltpu.VMEM)),
        scratch_shapes=[
            pltpu.VMEM((order, order), jnp.bfloat16),
            pltpu.VMEM((nb, order), jnp.bfloat16),
            pltpu.VMEM((nb, order), jnp.float32),
            pltpu.VMEM((cycle_size, 8, nb), jnp.float32),
            dma((4,)), dma, dma,
            six, six, six, six, three, three,
            six, six, six, six, three, three,
            seven, seven,
        ],
        compiler_params=pltpu.CompilerParams(
            collective_id=0, has_side_effects=True, vmem_limit_bytes=50 * 2**20,
        ),
    )(hamiltonian)
    return (sign_next, occupation[0, :1])


def solution(mesh):
    plane = PLANE[0] * PLANE[1] * PLANE[2]
    shards = symmetric_shards if mesh.shape["row"] == plane else gathered_shards
    placed = (P(("ka", "row"), None),)
    return jax.shard_map(
        shards,
        mesh=mesh,
        in_specs=placed,
        out_specs=(P(("ka", "row"), None), P("ka")),
        check_vma=False,
    )
```
